32 devices in a mesh: blk: 32 (over z, y, x, core).
Axes of the slice: x: 2, y: 2, z: 4, core: 2. Of those that a mesh axis runs over, the one named last changes fastest.
Arguments:
- adjacency: int32 [8192, 1280], P('blk'), may hold values 0 or 1
- weight: bfloat16 [8192, 1280], P('blk'), may hold values from -6 to 6
Outputs:
- closure: float32 [8192, 4352], P('blk')
The draws below stay inside these ranges and needn't reach their ends.
All inputs are finite; a program needn't handle non-finite values. No bound on the sum of `adjacency` on one device may be relied on, other than what follows from the above.
Results may differ from the reference program's by a relative error of at most 0.0041.
Values may be sent and summed in bfloat16 or wider, within the bound.
A program may use at most 64 MiB of HBM per device.

```python
import math
import jax
import jax.numpy as jnp
from jax import lax

B = 512
R = 256
K = 2
N = 8192


def place_ends(array, stream_key, least, largest):
    index_at = [jax.random.randint(jax.random.fold_in(stream_key, axis), (), 0, length) for axis, length in enumerate(array.shape)]
    main_axis = array.shape.index(max(array.shape))
    next_to = index_at[:main_axis] + [(index_at[main_axis] + 1) % array.shape[main_axis]] + index_at[main_axis + 1:]
    return array.at[tuple(index_at)].set(least).at[tuple(next_to)].set(largest)


def block_levels(own_key, shape, cuts, smallest, high):
    def one(dim, blocks):
        steps = jax.random.uniform(jax.random.fold_in(jax.random.fold_in(own_key, 6), dim), (blocks,), jnp.float32, smallest / len(cuts), high / len(cuts))
        return jnp.repeat(jnp.exp(steps), shape[dim] // blocks).reshape((-1,) + (1,) * (len(shape) - dim - 1))

    factor_of = one(*cuts[0])
    for cut in cuts[1:]:
        factor_of = factor_of * one(*cut)
    return factor_of


def noise(own_key, shape, scale, most, pieces=(), dtype=jnp.bfloat16):
    values = jax.random.normal(own_key, shape, jnp.float32) * scale
    if len(pieces) > 0:
        values = block_levels(own_key, shape, pieces, -0.22, 0.18) * values
    return jnp.clip(values, min=-most, max=most).astype(dtype)


def setup_inputs(seed: int = 0) -> dict:
    streams_of = jax.random.split(jax.random.key(seed), 3)
    return {
        "adjacency": place_ends((jax.random.randint(streams_of[0], (N, (2 * K + 1) * R), 0, 2) < 1).astype(jnp.int32), jax.random.fold_in(streams_of[0], 1), 0, 1),
        "weight": noise(streams_of[1], (N, (2 * K + 1) * R), 1.0, 6.0, ((0, 32),)),
    }


def banded(adjacency, weight):
    reach = (adjacency.shape[1] // R - 1) // 2
    local_row = lax.broadcasted_iota(jnp.int32, adjacency.shape, 0) % R
    offset = lax.broadcasted_iota(jnp.int32, adjacency.shape, 1) - local_row - reach * R
    keep = (jnp.abs(offset) <= B) & ((adjacency == 1) | (offset == 0))
    return jnp.where(keep, weight, jnp.zeros_like(weight))

def square(matrix, scale):
    block_count = matrix.shape[0] // R
    width_cols = matrix.shape[1]
    reach = (width_cols // R - 1) // 2
    blocks = matrix.reshape(block_count, R, width_cols)
    result = jnp.zeros((block_count, R, (4 * reach + 1) * R), jnp.float32)
    for column in range(2 * reach + 1):
        neighbour = jnp.roll(blocks, -(column - reach), axis=0).astype(jnp.float32)
        left = blocks[:, :, column * R:(column + 1) * R].astype(jnp.float32)
        product = jnp.einsum('bij,bjk->bik', left, neighbour)
        result = result.at[:, :, column * R:column * R + width_cols].add(product)
    return (result * scale).reshape(block_count * R, (4 * reach + 1) * R)

def reference(adjacency, weight):
    matrix = banded(adjacency, weight)
    first = square(matrix, 1.0 / math.sqrt(B)).astype(jnp.bfloat16)
    return square(first, 1.0 / math.sqrt(2 * B))
```

```python
import functools
import math

import jax
import jax.numpy as jnp
from jax import lax
from jax.experimental import pallas as pl
from jax.experimental.pallas import tpu as pltpu
from jax.sharding import PartitionSpec as P

B = 512
MESH = pl.DeviceIdType.MESH
CORES = 2
PLANE = 4
SPAN = PLANE - 1
LANES = 128
PAD = 16
CUTS = (128, 256, 512, 768, 1024, 1280, 1536, 1792)
ENDS = (4, 8, 12, 15, 16)


def block_of(buf, tri, at, k, rows):
    if k in (0, 4):
        return tri[at, k // 4]
    low = 2 * k * rows
    return jnp.concatenate([buf[at, low : low + rows, :], buf[at, low + rows : low + 2 * rows, :]], axis=1)


def product(left, buf, tri, core, rows, reach, u):
    low, high = max(-reach, u - 2), min(reach, u + 2)
    right = jnp.concatenate(
        [block_of(buf, tri, m + 2 * SPAN + core, u - m + 2, rows) for m in range(low, high + 1)], axis=0
    )
    return jnp.dot(
        left[:, (low + reach) * rows : (high + reach + 1) * rows], right, preferred_element_type=jnp.float32
    )


def gather_kernel(
    n, rows, adjacency, weight, t_low, buf, tri, adj, wgt, row, p_low,
    own_send, pair_send, hop_send, side_send, recv, in_sem,
):
    me = lax.axis_index("blk")
    core = me % CORES
    place = (me // CORES) % PLANE
    group = me // (CORES * PLANE)
    groups = n // (CORES * PLANE)
    partner = me + 1 - 2 * core
    up = ((group + 1) % groups * PLANE + place) * CORES + core
    down = ((group + groups - 1) % groups * PLANE + place) * CORES + core
    x_mate = place + 1 - 2 * (place % 2)
    y_mate = (place + 2) % PLANE
    inner = (place + 1) // 2 % 2
    a_mate = (1 - inner) * x_mate + inner * y_mate
    b_mate = inner * x_mate + (1 - inner) * y_mate
    d_mate = SPAN - place

    def device(q):
        return (group * PLANE + q) * CORES + core

    def slot(chip_offset, c):
        return (chip_offset + SPAN) * CORES + c

    def is_above(q, p):
        return (q - p + PLANE) // PLANE

    def cross(q, p):
        return q - p + PLANE - 2 * PLANE * is_above(q, p)

    total = buf.shape[1]
    starts = (0,) + CUTS
    ends = CUTS + (total,)
    chunks = len(starts)
    bounds = [(s, e - s) for s, e in zip(starts, ends)]

    barrier = pltpu.get_barrier_semaphore()
    greeted = [partner, up, down, device(a_mate), device(b_mate)]
    for other in greeted:
        pl.semaphore_signal(barrier, inc=1, device_id=(other,), device_id_type=MESH)

    order = (1, 2, 3, 0, 4)
    loads = []
    for k in order:
        cols = pl.ds(k * rows, rows)
        pair_of = (
            pltpu.make_async_copy(adjacency.at[:, cols], adj.at[:, cols], in_sem.at[0, k]),
            pltpu.make_async_copy(weight.at[:, cols], wgt.at[:, cols], in_sem.at[1, k]),
        )
        for load in pair_of:
            load.start()
        loads.append(pair_of)

    center = slot(0, core)
    r = lax.broadcasted_iota(jnp.int32, (rows, rows), 0)
    c = lax.broadcasted_iota(jnp.int32, (rows, rows), 1)
    for k, pair_of in zip(order, loads):
        for load in pair_of:
            load.wait()
        cols = slice(k * rows, (k + 1) * rows)
        offset = c - r + (k - 2) * rows
        keep = (adj[:, cols] == 1) | (offset == 0)
        if k in (0, 4):
            keep &= jnp.abs(offset) <= B
        kept = jnp.where(keep, wgt[:, cols].astype(jnp.float32), 0.0)
        low = kept.astype(row.dtype)
        row[:, cols] = low
        if k in (1, 2, 3):
            buf[center, 2 * k * rows : (2 * k + 1) * rows, :] = low[:, :LANES]
            buf[center, (2 * k + 1) * rows : (2 * k + 2) * rows, :] = low[:, LANES:]
        elif k == 0:
            first = kept
        else:
            square = jnp.where(c >= r, first, kept).astype(row.dtype)
            buf[center, :rows, :] = square[:, :LANES]
            buf[center, rows : 2 * rows, :] = square[:, LANES:]
            diagonal = jnp.sum(jnp.where(c == r, kept, 0.0), axis=0, keepdims=True)
            tail = jnp.concatenate(
                [diagonal[:, :LANES], diagonal[:, LANES:], jnp.zeros((PAD - 2, LANES), jnp.float32)], axis=0
            )
            buf[center, 8 * rows :, :] = tail.astype(row.dtype)
    pl.semaphore_wait(barrier, len(greeted))

    def chunk(ref, j):
        return ref.at[pl.ds(bounds[j][0], bounds[j][1])]

    sent = []

    def send(source, sem, j, to, at):
        copy = pltpu.make_async_remote_copy(
            src_ref=chunk(source, j),
            dst_ref=chunk(buf.at[at], j),
            send_sem=sem,
            recv_sem=recv.at[at, j],
            device_id=(to,),
            device_id_type=MESH,
        )
        copy.start()
        sent.append(copy)

    def arrived(at, j):
        pltpu.make_async_copy(chunk(buf.at[center], j), chunk(buf.at[at], j), recv.at[at, j]).wait()

    def pair(index, at, j):
        send(buf.at[at], pair_send.at[index, j], j, partner, at)

    def hop(index, q, j):
        above = is_above(q, place)
        to = above * up + (1 - above) * down
        send(buf.at[slot(q - place, core)], hop_send.at[index, j], j, to, slot(cross(q, place), core))

    a_in, b_in, d_in = (slot(q - place, core) for q in (a_mate, b_mate, d_mate))
    a_far, b_far, d_far = (slot(cross(q, place), core) for q in (a_mate, b_mate, d_mate))

    mine = buf.at[center]
    for j in range(chunks):
        send(mine, own_send.at[0, j], j, device(b_mate), slot(place - b_mate, core))
        send(mine, own_send.at[1, j], j, device(a_mate), slot(place - a_mate, core))
    for j in range(chunks):
        send(mine, own_send.at[2, j], j, partner, center)

    def unpack(at):
        square = jnp.concatenate([buf[at, :rows, :], buf[at, rows : 2 * rows, :]], axis=1)
        diagonal = jnp.concatenate(
            [buf[at, 8 * rows : 8 * rows + 1, :], buf[at, 8 * rows + 1 : 8 * rows + 2, :]], axis=1
        )
        zero = jnp.zeros_like(square)
        tri[at, 0] = jnp.where(c >= r, square, zero)
        tri[at, 1] = jnp.where(c < r, square, jnp.where(c == r, diagonal, zero))

    def take_other(at):
        other = at + 1 - 2 * core
        for j in range(chunks):
            arrived(other, j)
        unpack(other)

    for j in range(chunks):
        arrived(b_in, j)
        hop(0, b_mate, j)
        pair(0, b_in, j)
        arrived(a_in, j)
        send(buf.at[a_in], side_send.at[0, j], j, device(b_mate), slot(a_mate - b_mate, core))
        pair(1, a_in, j)
    for j in range(chunks):
        hop(1, a_mate, j)
    for j in range(chunks):
        arrived(b_far, j)
        send(
            buf.at[b_far], side_send.at[1, j], j, device(a_mate),
            slot(cross(b_mate, place) + place - a_mate, core),
        )
        pair(2, b_far, j)
    for at in (center, a_in, b_in, b_far):
        unpack(at)
    for at in (center, a_in, b_in):
        take_other(at)
    for j in range(chunks):
        arrived(d_in, j)
        pair(3, d_in, j)
        arrived(a_far, j)
        pair(4, a_far, j)
        arrived(d_far, j)
        pair(5, d_far, j)
    for at in (d_in, a_far, d_far):
        unpack(at)
    for at in (b_far, d_in, a_far, d_far):
        take_other(at)

    scale = 1.0 / math.sqrt(B)
    for u in range(-4, 5):
        p_low[:, (u + 4) * rows : (u + 5) * rows] = (
            product(row, buf, tri, core, rows, 2, u) * scale
        ).astype(p_low.dtype)
    scale = 1.0 / math.sqrt(B) / math.sqrt(2 * B)
    for u in range(-6, 7):
        t_low[:, (u + 6) * rows : (u + 7) * rows] = (
            product(p_low, buf, tri, core, rows, 4, u) * scale
        ).astype(t_low.dtype)
    for copy in sent:
        copy.wait_send()


def last_kernel(rows, t_low, buf, tri, out, stage, out_sem):
    core = lax.axis_index("blk") % CORES
    writes = []
    done = 0
    for i, u in enumerate(range(-8, 9)):
        stage[:, i * rows : (i + 1) * rows] = product(t_low, buf, tri, core, rows, 6, u)
        if i in ENDS:
            cols = pl.ds(done * rows, (i + 1 - done) * rows)
            write = pltpu.make_async_copy(stage.at[:, cols], out.at[:, cols], out_sem.at[len(writes)])
            write.start()
            writes.append(write)
            done = i + 1
    for write in writes:
        write.wait()


def local(n, adjacency, weight):
    rows = adjacency.shape[0]
    slots = (2 * SPAN + 1) * CORES
    low = weight.dtype
    chunks = len(CUTS) + 1
    vmem = pl.BlockSpec(memory_space=pltpu.VMEM)
    hbm = pl.BlockSpec(memory_space=pltpu.HBM)
    t_low, buf, tri = pl.pallas_call(
        functools.partial(gather_kernel, n, rows),
        out_shape=(
            jax.ShapeDtypeStruct((rows, 13 * rows), low),
            jax.ShapeDtypeStruct((slots, 8 * rows + PAD, LANES), low),
            jax.ShapeDtypeStruct((slots, 2, rows, rows), low),
        ),
        in_specs=[hbm, hbm],
        out_specs=(vmem, vmem, vmem),
        scratch_shapes=[
            pltpu.VMEM(adjacency.shape, jnp.int32),
            pltpu.VMEM(weight.shape, low),
            pltpu.VMEM((rows, 5 * rows), low),
            pltpu.VMEM((rows, 9 * rows), low),
            pltpu.SemaphoreType.DMA((3, chunks)),
            pltpu.SemaphoreType.DMA((6, chunks)),
            pltpu.SemaphoreType.DMA((2, chunks)),
            pltpu.SemaphoreType.DMA((2, chunks)),
            pltpu.SemaphoreType.DMA((slots, chunks)),
            pltpu.SemaphoreType.DMA((2, 5)),
        ],
        compiler_params=pltpu.CompilerParams(
            collective_id=0, has_side_effects=True, vmem_limit_bytes=24 * 1024 * 1024
        ),
        name="gather",
    )(*(pltpu.with_memory_space_constraint(x, pltpu.HBM) for x in (adjacency, weight)))
    return pl.pallas_call(
        functools.partial(last_kernel, rows),
        out_shape=jax.ShapeDtypeStruct((rows, 17 * rows), jnp.float32),
        in_specs=[vmem, vmem, vmem],
        out_specs=hbm,
        scratch_shapes=[
            pltpu.VMEM((rows, 17 * rows), jnp.float32),
            pltpu.SemaphoreType.DMA((len(ENDS),)),
        ],
        compiler_params=pltpu.CompilerParams(vmem_limit_bytes=24 * 1024 * 1024),
        name="last",
    )(t_low, buf, tri)


def solution(mesh):
    in_specs = (P("blk", None), P("blk", None))
    out_specs = P("blk", None)
    n = mesh.shape["blk"]
    return jax.shard_map(
        functools.partial(local, n), mesh=mesh, in_specs=in_specs, out_specs=out_specs, check_vma=False
    )
```

```python
import functools
import math

import jax
import jax.numpy as jnp
from jax import lax
from jax.experimental import pallas as pl
from jax.experimental.pallas import tpu as pltpu
from jax.sharding import PartitionSpec as P

B = 512
MESH = pl.DeviceIdType.MESH
CORES = 2
PLANE = 4
SPAN = PLANE - 1
LANES = 128
PAD = 16
LOADS = 2
CUTS = (128, 256, 512, 768, 1024, 1280, 1536, 1792)
SENDS = 6

OUTER = (
    (
        ("b", "me", 0), ("a", "me", 0), ("b", "me", 1), ("a", "me", 1), ("b", "me", 2), ("a", "me", 2),
        ("b", "me", 3), ("a", "me", 3), ("b", "me", 4), ("a", "me", 4), ("b", "me", 5), ("a", "me", 5),
        ("b", "me", 6), ("a", "me", 6), ("b", "me", 7), ("a", "me", 7), ("b", "me", 8), ("a", "me", 8),
    ),
    (
        ("b", 0), ("zb", "b", 0), ("a", 0), ("b", "a", 0), ("b", 1), ("zb", "b", 1), ("a", 1), ("b", "a", 1),
        ("b", 2), ("zb", "b", 2), ("a", 2), ("b", "a", 2), ("b", 3), ("zb", "b", 3), ("a", 3), ("b", "a", 3),
        ("b", 4), ("zb", "b", 4), ("a", 4), ("b", "a", 4), ("b", 5), ("zb", "b", 5), ("a", 5), ("b", "a", 5),
        ("b", 6), ("zb", "b", 6), ("a", 6), ("b", "a", 6), ("b", 7), ("zb", "b", 7), ("a", 7), ("b", "a", 7),
        ("b", 8), ("zb", "b", 8), ("a", 8), ("b", "a", 8), ("za", "a", 0), ("za", "a", 1), ("za", "a", 2),
        ("za", "a", 3), ("za", "a", 4), ("za", "a", 5), ("za", "a", 6),
    ),
    (
        ("za", "a", 7), ("za", "a", 8), ("fb", 0), ("a", "fb", 0), ("fb", 1), ("a", "fb", 1), ("fb", 2),
        ("a", "fb", 2), ("fb", 3), ("a", "fb", 3), ("fb", 4), ("a", "fb", 4), ("fb", 5), ("a", "fb", 5), ("fb", 6),
        ("a", "fb", 6), ("fb", 7), ("a", "fb", 7), ("fb", 8), ("a", "fb", 8), ("d", 0), ("fa", 0), ("fd", 0),
        ("d", 1), ("fa", 1), ("fd", 1), ("d", 2), ("fa", 2), ("fd", 2), ("d", 3), ("fa", 3), ("fd", 3), ("d", 4),
        ("fa", 4), ("fd", 4), ("d", 5), ("fa", 5), ("fd", 5), ("d", 6), ("fa", 6), ("fd", 6), ("d", 7), ("fa", 7),
        ("fd", 7), ("d", 8), ("fa", 8), ("fd", 8),
    ),
    (
    ),
    (
    ),
    (
    ),
    (
    ),
    (
    ),
    (
    ),
    (
    ),
)
INNER = (
    (
        ("b", "me", 0), ("a", "me", 0), ("b", "me", 1), ("a", "me", 1), ("b", "me", 2), ("a", "me", 2),
        ("b", "me", 3), ("a", "me", 3), ("b", "me", 4), ("a", "me", 4), ("b", "me", 5), ("a", "me", 5),
        ("b", "me", 6), ("a", "me", 6), ("b", "me", 7), ("a", "me", 7), ("b", "me", 8), ("a", "me", 8),
    ),
    (
        ("b", 0), ("zb", "b", 0), ("a", 0), ("b", "a", 0), ("b", 1), ("zb", "b", 1), ("a", 1), ("b", "a", 1),
        ("b", 2), ("zb", "b", 2), ("a", 2), ("b", "a", 2), ("b", 3), ("zb", "b", 3), ("a", 3), ("b", "a", 3),
        ("b", 4), ("zb", "b", 4), ("a", 4), ("b", "a", 4), ("b", 5), ("zb", "b", 5), ("a", 5), ("b", "a", 5),
        ("b", 6), ("zb", "b", 6), ("a", 6), ("b", "a", 6), ("b", 7), ("zb", "b", 7), ("a", 7), ("b", "a", 7),
        ("b", 8), ("zb", "b", 8), ("a", 8), ("b", "a", 8), ("za", "a", 0), ("za", "a", 1), ("za", "a", 2),
        ("za", "a", 3), ("za", "a", 4), ("za", "a", 5), ("za", "a", 6),
    ),
    (
        ("za", "a", 7), ("za", "a", 8), ("fb", 0), ("a", "fb", 0), ("fb", 1), ("a", "fb", 1), ("fb", 2),
        ("a", "fb", 2), ("fb", 3), ("a", "fb", 3), ("fb", 4), ("a", "fb", 4), ("fb", 5), ("a", "fb", 5), ("fb", 6),
        ("a", "fb", 6), ("fb", 7), ("a", "fb", 7), ("fb", 8), ("a", "fb", 8), ("d", 0), ("fa", 0), ("fd", 0),
        ("d", 1), ("fa", 1), ("fd", 1), ("d", 2), ("fa", 2), ("fd", 2), ("d", 3), ("fa", 3), ("fd", 3), ("d", 4),
        ("fa", 4), ("fd", 4), ("d", 5), ("fa", 5), ("fd", 5), ("d", 6), ("fa", 6), ("fd", 6), ("d", 7), ("fa", 7),
        ("fd", 7), ("d", 8), ("fa", 8),
    ),
    (
    ),
    (
    ),
    (
    ),
    (
    ),
    (
    ),
    (
    ),
    (
        ("fd", 8),
    ),
)
SPANS = ((-8, -5), (-5, -2), (3, 6), (6, 9))


def block_of(buf, tri, at, k, rows):
    if k in (0, 4):
        return tri[at, k // 4]
    low = 2 * k * rows
    return jnp.concatenate([buf[at, low : low + rows, :], buf[at, low + rows : low + 2 * rows, :]], axis=1)


def ends_of(buf, at, rows):
    r = lax.broadcasted_iota(jnp.int32, (rows, rows), 0)
    c = lax.broadcasted_iota(jnp.int32, (rows, rows), 1)
    square = jnp.concatenate([buf[at, :rows, :], buf[at, rows : 2 * rows, :]], axis=1)
    diagonal = jnp.concatenate(
        [buf[at, 8 * rows : 8 * rows + 1, :], buf[at, 8 * rows + 1 : 8 * rows + 2, :]], axis=1
    )
    zero = jnp.zeros_like(square)
    return jnp.where(c >= r, square, zero), jnp.where(c < r, square, jnp.where(c == r, diagonal, zero))


def product(left, buf, tri, core, rows, reach, u, only):
    terms = [m for m in only if abs(u - m) <= 2]
    right = jnp.concatenate([block_of(buf, tri, m + 2 * SPAN + core, u - m + 2, rows) for m in terms], axis=0)
    low, high = terms[0] + reach, terms[-1] + reach
    return jnp.dot(left[:, low * rows : (high + 1) * rows], right, preferred_element_type=jnp.float32)


def gather_kernel(
    n, rows, adjacency, weight, t_low, partial, buf, adj, wgt, row, p_low, tri, via,
    send_sem, pair_send, recv, pair_recv, via_recv, in_sem,
):
    me = lax.axis_index("blk")
    core = me % CORES
    place = (me // CORES) % PLANE
    group = me // (CORES * PLANE)
    groups = n // (CORES * PLANE)
    partner = me + 1 - 2 * core
    up = ((group + 1) % groups * PLANE + place) * CORES + core
    down = ((group + groups - 1) % groups * PLANE + place) * CORES + core
    x_mate = place + 1 - 2 * (place % 2)
    y_mate = (place + 2) % PLANE
    inner = (place + 1) // 2 % 2
    a_mate = (1 - inner) * x_mate + inner * y_mate
    b_mate = inner * x_mate + (1 - inner) * y_mate
    d_mate = SPAN - place

    def device(q):
        return (group * PLANE + q) * CORES + core

    def is_above(q, p):
        return (q - p + PLANE) // PLANE

    def cross(q, p):
        return q - p + PLANE - 2 * PLANE * is_above(q, p)

    def either(outer_one, inner_one):
        return outer_one + inner * (inner_one - outer_one)

    def beyond(q):
        above = is_above(q, place)
        return above * up + (1 - above) * down

    total = buf.shape[1]
    bounds = [(s, e - s) for s, e in zip((0,) + CUTS, CUTS + (total,))]
    chunks = range(len(bounds))

    mates = {"a": a_mate, "b": b_mate, "d": d_mate}
    chip = {"me": 0 * place}
    for name, q in mates.items():
        chip[name] = q - place
        chip["f" + name] = cross(q, place)
    device_of = {"a": device(a_mate), "b": device(b_mate)}
    for name, q in mates.items():
        device_of["z" + name] = beyond(q)
    device_of["k0"] = up + down - device_of["zb"]
    device_of["k1"] = up + down - device_of["za"]
    place_of = {"a": place - a_mate, "b": place - b_mate}
    own_via = {m: cross(place, mates[m]) for m in ("a", "b")}

    def slot(chip_offset):
        return (chip_offset + SPAN) * CORES + core

    barrier = pltpu.get_barrier_semaphore()
    greeted = [partner, up, down, device_of["a"], device_of["b"]]
    for other in greeted:
        pl.semaphore_signal(barrier, inc=1, device_id=(other,), device_id_type=MESH)

    step = rows // LOADS
    loads = []
    for i in range(LOADS):
        part = pl.ds(i * step, step)
        loads.append((
            pltpu.make_async_copy(adjacency.at[part], adj.at[part], in_sem.at[0, i]),
            pltpu.make_async_copy(weight.at[part], wgt.at[part], in_sem.at[1, i]),
        ))
    for pair_of in loads:
        for load in pair_of:
            load.start()

    center = slot(0)
    diagonal = jnp.zeros((1, rows), jnp.float32)
    for i, pair_of in enumerate(loads):
        for load in pair_of:
            load.wait()
        part = slice(i * step, (i + 1) * step)
        r = lax.broadcasted_iota(jnp.int32, (step, rows), 0) + i * step
        c = lax.broadcasted_iota(jnp.int32, (step, rows), 1)
        kept = []
        for k in range(5):
            cols = slice(k * rows, (k + 1) * rows)
            keep = adj[part, cols] == 1
            if k == 0:
                keep &= c >= r
            elif k == 2:
                keep |= c == r
            elif k == 4:
                keep &= c <= r
            kept.append(jnp.where(keep, wgt[part, cols].astype(jnp.float32), 0.0))
            row[part, cols] = kept[k].astype(row.dtype)
        packed = [jnp.where(c >= r, kept[0], kept[4])] + kept[1:4]
        for k in range(4):
            low = packed[k].astype(row.dtype)
            for h in range(2):
                start = (2 * k + h) * rows + i * step
                buf[center, start : start + step, :] = low[:, h * LANES : (h + 1) * LANES]
        diagonal += jnp.sum(jnp.where(c == r, kept[4], 0.0), axis=0, keepdims=True)
    tail = jnp.concatenate(
        [diagonal[:, :LANES], diagonal[:, LANES:], jnp.zeros((PAD - 2, LANES), jnp.float32)], axis=0
    )
    buf[center, 8 * rows :, :] = tail.astype(row.dtype)
    pl.semaphore_wait(barrier, len(greeted))

    def chunk(at, j):
        return buf.at[at, pl.ds(bounds[j][0], bounds[j][1])]

    def arrive(chip_offset, j):
        return recv.at[chip_offset + SPAN, j]

    def remote(source, target, sem, arrival, to):
        return pltpu.make_async_remote_copy(
            src_ref=source, dst_ref=target, send_sem=sem, recv_sem=arrival, device_id=(to,), device_id_type=MESH
        )

    def pair(chip_offset, j):
        at = slot(chip_offset)
        remote(chunk(at, j), chunk(at, j), pair_send, pair_recv.at[chip_offset + SPAN], partner).start()

    classes = []
    sent = ({}, {})

    def send(kind, link, name, j):
        key = (link, name)
        if key not in classes:
            classes.append(key)
        sem = send_sem.at[classes.index(key)]
        sent[kind][key] = sent[kind].get(key, 0) + bounds[j][1]
        to = device_of[link]
        if link[0] == "k":
            i = int(link[1])
            remote(chunk(center, j), via.at[i], sem, via_recv.at[i], to).start()
        elif name[0] == "v":
            there = own_via[link]
            remote(via.at[int(name[1])], chunk(slot(there), j), sem, arrive(there, j), to).start()
        else:
            there = chip["f" + name] if link[0] == "z" else chip[name] + place_of[link]
            remote(chunk(slot(chip[name]), j), chunk(slot(there), j), sem, arrive(there, j), to).start()

    def take(name, j):
        if name[0] == "v":
            i = int(name[1])
            pltpu.make_async_copy(chunk(center, j), via.at[i], via_recv.at[i]).wait()
            return
        at = slot(chip[name])
        pltpu.make_async_copy(chunk(center, j), chunk(at, j), arrive(chip[name], j)).wait()
        pair(chip[name], j)

    def perform(index):
        for kind, steps in enumerate((OUTER, INNER)):
            def body(kind=kind, steps=steps):
                for op in steps[index]:
                    if len(op) == 2:
                        take(*op)
                    else:
                        send(kind, *op)

            pl.when(inner == kind)(body)

    def take_other(chip_offset):
        at = slot(chip_offset) + 1 - 2 * core
        pltpu.make_async_copy(buf.at[center], buf.at[at], pair_recv.at[chip_offset + SPAN]).wait()

    def unpack(at):
        tri[at, 0], tri[at, 1] = ends_of(buf, at, rows)

    near = ("me", "a", "b")
    near_z, near_plane = either(chip["fb"], chip["fa"]), either(chip["fd"], chip["d"])
    far_z, far_plane = either(chip["fa"], chip["fb"]), either(chip["d"], chip["fd"])

    perform(0)
    for j in chunks:
        pair(chip["me"], j)
    unpack(center)
    perform(1)
    for name in near:
        if name != "me":
            unpack(slot(chip[name]))
        take_other(chip[name])
        unpack(slot(chip[name]) + 1 - 2 * core)
    perform(2)
    for offset in (near_z, near_plane):
        unpack(slot(offset))
        take_other(offset)
        unpack(slot(offset) + 1 - 2 * core)

    scale = 1.0 / math.sqrt(B)
    for u in range(-4, 5):
        p_low[:, (u + 4) * rows : (u + 5) * rows] = (
            product(row, buf, tri, core, rows, 2, u, range(-2, 3)) * scale
        ).astype(p_low.dtype)
    perform(3)
    scale = 1.0 / math.sqrt(B) / math.sqrt(2 * B)
    for u in range(-6, 7):
        t_low[:, (u + 6) * rows : (u + 7) * rows] = (
            product(p_low, buf, tri, core, rows, 4, u, range(-4, 5)) * scale
        ).astype(t_low.dtype)
        if u in (-2, 2, 6):
            perform({-2: 4, 2: 5, 6: 6}[u])
    for u in range(-6, 7):
        partial[:, (u + 6) * rows : (u + 7) * rows] = product(t_low, buf, tri, core, rows, 6, u, range(-4, 5))
        if u in (-2, 2, 6):
            perform({-2: 7, 2: 8, 6: 9}[u])
    for offset in (far_z, far_plane):
        take_other(offset)

    def sent_out(size, sem):
        part = buf.at[center, pl.ds(0, size)]
        remote(part, part, sem, via_recv.at[0], partner).wait_send()

    blocks = buf.at[pl.ds(0, 2 * SPAN + 1)]
    remote(blocks, blocks, pair_send, via_recv.at[0], partner).wait_send()
    for kind in range(2):
        def finish(kind=kind):
            for key, size in sent[kind].items():
                sent_out(size, send_sem.at[classes.index(key)])

        pl.when(inner == kind)(finish)


def last_kernel(rows, t_low, partial, buf, out, tri, stage, out_sem):
    core = lax.axis_index("blk") % CORES
    far = (-6, -5, 5, 6)
    middle = pl.ds(6 * rows, 5 * rows)
    writes = [pltpu.make_async_copy(partial.at[:, pl.ds(4 * rows, 5 * rows)], out.at[:, middle], out_sem.at[0])]
    writes[0].start()
    for i, m in enumerate(far):
        tri[i, 0], tri[i, 1] = ends_of(buf, m + 2 * SPAN + core, rows)
    for low, high in SPANS:
        for u in range(low, high):
            terms = [(i, m) for i, m in enumerate(far) if abs(u - m) <= 2]
            right = []
            for i, m in terms:
                k = u - m + 2
                at = m + 2 * SPAN + core
                right.append(tri[i, k // 4] if k in (0, 4) else block_of(buf, None, at, k, rows))
            first, last = terms[0][1] + 6, terms[-1][1] + 6
            value = jnp.dot(
                t_low[:, first * rows : (last + 1) * rows], jnp.concatenate(right, axis=0),
                preferred_element_type=jnp.float32,
            )
            if abs(u) <= 6:
                value += partial[:, (u + 6) * rows : (u + 7) * rows]
            stage[:, (u + 8) * rows : (u + 9) * rows] = value
        cols = pl.ds((low + 8) * rows, (high - low) * rows)
        write = pltpu.make_async_copy(stage.at[:, cols], out.at[:, cols], out_sem.at[len(writes)])
        write.start()
        writes.append(write)
    for write in writes:
        write.wait()


def local(n, adjacency, weight):
    rows = adjacency.shape[0]
    slots = (2 * SPAN + 1) * CORES
    low = weight.dtype
    chunks = len(CUTS) + 1
    vmem = pl.BlockSpec(memory_space=pltpu.VMEM)
    hbm = pl.BlockSpec(memory_space=pltpu.HBM)
    t_low, partial, buf = pl.pallas_call(
        functools.partial(gather_kernel, n, rows),
        out_shape=(
            jax.ShapeDtypeStruct((rows, 13 * rows), low),
            jax.ShapeDtypeStruct((rows, 13 * rows), jnp.float32),
            jax.ShapeDtypeStruct((slots, 8 * rows + PAD, LANES), low),
        ),
        in_specs=[hbm, hbm],
        out_specs=(vmem, vmem, vmem),
        scratch_shapes=[
            pltpu.VMEM(adjacency.shape, jnp.int32),
            pltpu.VMEM(weight.shape, low),
            pltpu.VMEM((rows, 5 * rows), low),
            pltpu.VMEM((rows, 9 * rows), low),
            pltpu.VMEM((slots, 2, rows, rows), low),
            pltpu.VMEM((2, CUTS[0], LANES), low),
            pltpu.SemaphoreType.DMA((SENDS,)),
            pltpu.SemaphoreType.DMA,
            pltpu.SemaphoreType.DMA((2 * SPAN + 1, chunks)),
            pltpu.SemaphoreType.DMA((2 * SPAN + 1,)),
            pltpu.SemaphoreType.DMA((2,)),
            pltpu.SemaphoreType.DMA((2, LOADS)),
        ],
        compiler_params=pltpu.CompilerParams(
            collective_id=0, has_side_effects=True, vmem_limit_bytes=24 * 1024 * 1024
        ),
        name="gather",
    )(*(pltpu.with_memory_space_constraint(x, pltpu.HBM) for x in (adjacency, weight)))
    return pl.pallas_call(
        functools.partial(last_kernel, rows),
        out_shape=jax.ShapeDtypeStruct((rows, 17 * rows), jnp.float32),
        in_specs=[vmem, vmem, vmem],
        out_specs=hbm,
        scratch_shapes=[
            pltpu.VMEM((4, 2, rows, rows), low),
            pltpu.VMEM((rows, 17 * rows), jnp.float32),
            pltpu.SemaphoreType.DMA((len(SPANS) + 1,)),
        ],
        compiler_params=pltpu.CompilerParams(vmem_limit_bytes=24 * 1024 * 1024),
        name="last",
    )(t_low, partial, buf)


def solution(mesh):
    in_specs = (P("blk", None), P("blk", None))
    out_specs = P("blk", None)
    n = mesh.shape["blk"]
    return jax.shard_map(
        functools.partial(local, n), mesh=mesh, in_specs=in_specs, out_specs=out_specs, check_vma=False
    )
```

```python
import functools
import math

import jax
import jax.numpy as jnp
from jax import lax
from jax.experimental import pallas as pl
from jax.experimental.pallas import tpu as pltpu
from jax.sharding import PartitionSpec as P

B = 512
MESH = pl.DeviceIdType.MESH
CORES = 2
PLANE = 4
SPAN = PLANE - 1
LANES = 128
PAD = 16
LOADS = 2
CUTS = (256, 512, 768, 1024, 1280, 1536, 1792)
LAG = 3
SENT_BLOCKS = 2 + 2 + 2 + (2 * SPAN + 1)
FORWARDS_T = {-2: (0, 1), 2: (2, 3), 6: (4,)}
FORWARDS_OUT = {-2: (5,), 2: (6,), 6: (7,)}
SPANS = ((-8, -5), (-5, -2), (3, 6), (6, 9))


def block_of(buf, tri, at, k, rows):
    if k in (0, 4):
        return tri[at, k // 4]
    low = 2 * k * rows
    return jnp.concatenate([buf[at, low : low + rows, :], buf[at, low + rows : low + 2 * rows, :]], axis=1)


def ends_of(buf, at, rows):
    r = lax.broadcasted_iota(jnp.int32, (rows, rows), 0)
    c = lax.broadcasted_iota(jnp.int32, (rows, rows), 1)
    square = jnp.concatenate([buf[at, :rows, :], buf[at, rows : 2 * rows, :]], axis=1)
    diagonal = jnp.concatenate(
        [buf[at, 8 * rows : 8 * rows + 1, :], buf[at, 8 * rows + 1 : 8 * rows + 2, :]], axis=1
    )
    zero = jnp.zeros_like(square)
    return jnp.where(c >= r, square, zero), jnp.where(c < r, square, jnp.where(c == r, diagonal, zero))


def product(left, buf, tri, core, rows, reach, u, only):
    terms = [m for m in only if abs(u - m) <= 2]
    right = jnp.concatenate([block_of(buf, tri, m + 2 * SPAN + core, u - m + 2, rows) for m in terms], axis=0)
    low, high = terms[0] + reach, terms[-1] + reach
    return jnp.dot(left[:, low * rows : (high + 1) * rows], right, preferred_element_type=jnp.float32)


def gather_kernel(
    n, rows, adjacency, weight, t_low, partial, buf, adj, wgt, row, p_low, tri,
    send_sem, recv, pair_recv, in_sem,
):
    me = lax.axis_index("blk")
    core = me % CORES
    place = (me // CORES) % PLANE
    group = me // (CORES * PLANE)
    groups = n // (CORES * PLANE)
    partner = me + 1 - 2 * core
    up = ((group + 1) % groups * PLANE + place) * CORES + core
    down = ((group + groups - 1) % groups * PLANE + place) * CORES + core
    x_mate = place + 1 - 2 * (place % 2)
    y_mate = (place + 2) % PLANE
    d_mate = SPAN - place
    inner = (place + 1) // 2 % 2

    def device(q):
        return (group * PLANE + q) * CORES + core

    def is_above(q, p):
        return (q - p + PLANE) // PLANE

    def cross(q, p):
        return q - p + PLANE - 2 * PLANE * is_above(q, p)

    def either(outer_one, inner_one):
        return outer_one + inner * (inner_one - outer_one)

    def slot(offset):
        return (offset + SPAN) * CORES + core

    total = buf.shape[1]
    bounds = [(s, e - s) for s, e in zip((0,) + CUTS, CUTS + (total,))]
    chunks = range(len(bounds))
    x_dev, y_dev = device(x_mate), device(y_mate)

    barrier = pltpu.get_barrier_semaphore()
    greeted = [partner, up, down, x_dev, y_dev]
    for other in greeted:
        pl.semaphore_signal(barrier, inc=1, device_id=(other,), device_id_type=MESH)

    step = rows // LOADS
    loads = []
    for i in range(LOADS):
        part = pl.ds(i * step, step)
        loads.append((
            pltpu.make_async_copy(adjacency.at[part], adj.at[part], in_sem.at[0, i]),
            pltpu.make_async_copy(weight.at[part], wgt.at[part], in_sem.at[1, i]),
        ))
    for pair_of in loads:
        for load in pair_of:
            load.start()

    center = slot(0)
    diagonal = jnp.zeros((1, rows), jnp.float32)
    for i, pair_of in enumerate(loads):
        for load in pair_of:
            load.wait()
        part = slice(i * step, (i + 1) * step)
        r = lax.broadcasted_iota(jnp.int32, (step, rows), 0) + i * step
        c = lax.broadcasted_iota(jnp.int32, (step, rows), 1)
        kept = []
        for k in range(5):
            cols = slice(k * rows, (k + 1) * rows)
            keep = adj[part, cols] == 1
            if k == 0:
                keep &= c >= r
            elif k == 2:
                keep |= c == r
            elif k == 4:
                keep &= c <= r
            kept.append(jnp.where(keep, wgt[part, cols].astype(jnp.float32), 0.0))
            row[part, cols] = kept[k].astype(row.dtype)
        packed = [jnp.where(c >= r, kept[0], kept[4])] + kept[1:4]
        for k in range(4):
            low = packed[k].astype(row.dtype)
            for h in range(2):
                start = (2 * k + h) * rows + i * step
                buf[center, start : start + step, :] = low[:, h * LANES : (h + 1) * LANES]
        diagonal += jnp.sum(jnp.where(c == r, kept[4], 0.0), axis=0, keepdims=True)
    tail = jnp.concatenate(
        [diagonal[:, :LANES], diagonal[:, LANES:], jnp.zeros((PAD - 2, LANES), jnp.float32)], axis=0
    )
    buf[center, 8 * rows :, :] = tail.astype(row.dtype)
    pl.semaphore_wait(barrier, len(greeted))

    def chunk(offset, j):
        return buf.at[slot(offset), pl.ds(bounds[j][0], bounds[j][1])]

    def arrival(offset, j):
        return recv.at[offset + SPAN - (offset + SPAN) // (SPAN + 1), j]

    def remote(source, target, sem, to):
        return pltpu.make_async_remote_copy(
            src_ref=source, dst_ref=target, send_sem=send_sem, recv_sem=sem, device_id=(to,), device_id_type=MESH
        )

    def send(offset, j, to, there):
        remote(chunk(offset, j), chunk(there, j), arrival(there, j), to).start()

    def pair(offset, j):
        remote(chunk(offset, j), chunk(offset, j), pair_recv.at[offset + SPAN], partner).start()

    def take(offset, j):
        pltpu.make_async_copy(chunk(0, j), chunk(offset, j), arrival(offset, j)).wait()

    def take_pair(offset, j):
        take(offset, j)
        pair(offset, j)

    def hop(q, j):
        above = is_above(q, place)
        send(q - place, j, above * up + (1 - above) * down, cross(q, place))

    def other(offset):
        return slot(offset) + 1 - 2 * core

    def unpack(at):
        tri[at, 0], tri[at, 1] = ends_of(buf, at, rows)

    def unpack_own(offset):
        unpack(slot(offset))

    def unpack_other(offset):
        at = other(offset)
        pltpu.make_async_copy(buf.at[center], buf.at[at], pair_recv.at[offset + SPAN]).wait()
        unpack(at)

    x, y, d = (q - place for q in (x_mate, y_mate, d_mate))
    x_far, y_far, d_far = (cross(q, place) for q in (x_mate, y_mate, d_mate))
    near, far = either(d_far, d), either(d, d_far)

    for j in chunks:
        send(0, j, y_dev, place - y_mate)
        send(0, j, x_dev, place - x_mate)
    for j in chunks:
        pair(0, j)
    unpack_own(0)
    def relay_far(j):
        take(y_far, j)
        send(y_far, j, x_dev, y_far + place - x_mate)
        pair(y_far, j)

    for j in chunks:
        take(y, j)
        hop(y_mate, j)
        pair(y, j)
        take(x, j)
        send(x, j, y_dev, x_mate - y_mate)
        pair(x, j)
        if j >= LAG:
            relay_far(j - LAG)
    for j in chunks:
        hop(x_mate, j)
    for j in chunks[-LAG:]:
        relay_far(j)
    unpack_other(0)
    for offset in (x, y, y_far):
        unpack_own(offset)
        unpack_other(offset)
    for j in chunks:
        take_pair(near, j)
    for j in chunks[:4]:
        take_pair(far, j)
    unpack_own(near)
    unpack_other(near)

    scale = 1.0 / math.sqrt(B)
    for u in range(-4, 5):
        p_low[:, (u + 4) * rows : (u + 5) * rows] = (
            product(row, buf, tri, core, rows, 2, u, range(-2, 3)) * scale
        ).astype(p_low.dtype)
    for j in chunks[4:]:
        take_pair(far, j)
    scale = 1.0 / math.sqrt(B) / math.sqrt(2 * B)
    for u in range(-6, 7):
        t_low[:, (u + 6) * rows : (u + 7) * rows] = (
            product(p_low, buf, tri, core, rows, 4, u, range(-4, 5)) * scale
        ).astype(t_low.dtype)
        for j in FORWARDS_T.get(u, ()):
            take_pair(x_far, j)
    for u in range(-6, 7):
        partial[:, (u + 6) * rows : (u + 7) * rows] = product(t_low, buf, tri, core, rows, 6, u, range(-4, 5))
        for j in FORWARDS_OUT.get(u, ()):
            take_pair(x_far, j)
    for offset in (far, x_far):
        pltpu.make_async_copy(buf.at[center], buf.at[other(offset)], pair_recv.at[offset + SPAN]).wait()
    blocks = buf.at[pl.ds(0, SENT_BLOCKS)]
    remote(blocks, blocks, pair_recv.at[0], partner).wait_send()


def last_kernel(rows, t_low, partial, buf, out, tri, stage, out_sem):
    core = lax.axis_index("blk") % CORES
    far = (-6, -5, 5, 6)
    middle = pl.ds(6 * rows, 5 * rows)
    writes = [pltpu.make_async_copy(partial.at[:, pl.ds(4 * rows, 5 * rows)], out.at[:, middle], out_sem.at[0])]
    writes[0].start()
    for i, m in enumerate(far):
        tri[i, 0], tri[i, 1] = ends_of(buf, m + 2 * SPAN + core, rows)
    for low, high in SPANS:
        for u in range(low, high):
            terms = [(i, m) for i, m in enumerate(far) if abs(u - m) <= 2]
            right = []
            for i, m in terms:
                k = u - m + 2
                at = m + 2 * SPAN + core
                right.append(tri[i, k // 4] if k in (0, 4) else block_of(buf, None, at, k, rows))
            first, last = terms[0][1] + 6, terms[-1][1] + 6
            value = jnp.dot(
                t_low[:, first * rows : (last + 1) * rows], jnp.concatenate(right, axis=0),
                preferred_element_type=jnp.float32,
            )
            if abs(u) <= 6:
                value += partial[:, (u + 6) * rows : (u + 7) * rows]
            stage[:, (u + 8) * rows : (u + 9) * rows] = value
        cols = pl.ds((low + 8) * rows, (high - low) * rows)
        write = pltpu.make_async_copy(stage.at[:, cols], out.at[:, cols], out_sem.at[len(writes)])
        write.start()
        writes.append(write)
    for write in writes:
        write.wait()


def local(n, adjacency, weight):
    rows = adjacency.shape[0]
    slots = (2 * SPAN + 1) * CORES
    low = weight.dtype
    chunks = len(CUTS) + 1
    vmem = pl.BlockSpec(memory_space=pltpu.VMEM)
    hbm = pl.BlockSpec(memory_space=pltpu.HBM)
    t_low, partial, buf = pl.pallas_call(
        functools.partial(gather_kernel, n, rows),
        out_shape=(
            jax.ShapeDtypeStruct((rows, 13 * rows), low),
            jax.ShapeDtypeStruct((rows, 13 * rows), jnp.float32),
            jax.ShapeDtypeStruct((slots, 8 * rows + PAD, LANES), low),
        ),
        in_specs=[hbm, hbm],
        out_specs=(vmem, vmem, vmem),
        scratch_shapes=[
            pltpu.VMEM(adjacency.shape, jnp.int32),
            pltpu.VMEM(weight.shape, low),
            pltpu.VMEM((rows, 5 * rows), low),
            pltpu.VMEM((rows, 9 * rows), low),
            pltpu.VMEM((slots, 2, rows, rows), low),
            pltpu.SemaphoreType.DMA,
            pltpu.SemaphoreType.DMA((2 * SPAN, chunks)),
            pltpu.SemaphoreType.DMA((2 * SPAN + 1,)),
            pltpu.SemaphoreType.DMA((2, LOADS)),
        ],
        compiler_params=pltpu.CompilerParams(
            collective_id=0, has_side_effects=True, vmem_limit_bytes=24 * 1024 * 1024
        ),
        name="gather",
    )(*(pltpu.with_memory_space_constraint(x, pltpu.HBM) for x in (adjacency, weight)))
    return pl.pallas_call(
        functools.partial(last_kernel, rows),
        out_shape=jax.ShapeDtypeStruct((rows, 17 * rows), jnp.float32),
        in_specs=[vmem, vmem, vmem],
        out_specs=hbm,
        scratch_shapes=[
            pltpu.VMEM((4, 2, rows, rows), low),
            pltpu.VMEM((rows, 17 * rows), jnp.float32),
            pltpu.SemaphoreType.DMA((len(SPANS) + 1,)),
        ],
        compiler_params=pltpu.CompilerParams(vmem_limit_bytes=24 * 1024 * 1024),
        name="last",
    )(t_low, partial, buf)


def solution(mesh):
    in_specs = (P("blk", None), P("blk", None))
    out_specs = P("blk", None)
    n = mesh.shape["blk"]
    return jax.shard_map(
        functools.partial(local, n), mesh=mesh, in_specs=in_specs, out_specs=out_specs, check_vma=False
    )
```

```python
import functools
import math

import jax
import jax.numpy as jnp
from jax import lax
from jax.experimental import pallas as pl
from jax.experimental.pallas import tpu as pltpu
from jax.sharding import PartitionSpec as P

B = 512
MESH = pl.DeviceIdType.MESH
CORES = 2
PLANE = 4
SPAN = PLANE - 1
LANES = 128
PAD = 16
LOADS = 2
CUTS = (256, 512, 768, 1024, 1280, 1536, 1792)
LAG = 3
SENT_BLOCKS = 2 + 2 + 2 + (2 * SPAN + 1)
FORWARDS = (
    ((0, 0), (0, 1), (0, 2), (0, 3), (1, 1), (1, 2), (1, 3)),
    ((0, 4), (0, 5), (0, 6), (0, 7), (1, 4)),
)
FORWARDS_T = {-3: ((1, 5),), 0: ((1, 6),), 3: ((1, 0), (1, 7))}
FORWARDS_OUT = {}
SPANS = ((-8, -5), (-5, -2), (3, 6), (6, 9))


def block_of(buf, tri, at, k, rows):
    if k in (0, 4):
        return tri[at, k // 4]
    low = 2 * k * rows
    return jnp.concatenate([buf[at, low : low + rows, :], buf[at, low + rows : low + 2 * rows, :]], axis=1)


def ends_of(buf, at, rows):
    r = lax.broadcasted_iota(jnp.int32, (rows, rows), 0)
    c = lax.broadcasted_iota(jnp.int32, (rows, rows), 1)
    square = jnp.concatenate([buf[at, :rows, :], buf[at, rows : 2 * rows, :]], axis=1)
    diagonal = jnp.concatenate(
        [buf[at, 8 * rows : 8 * rows + 1, :], buf[at, 8 * rows + 1 : 8 * rows + 2, :]], axis=1
    )
    zero = jnp.zeros_like(square)
    return jnp.where(c >= r, square, zero), jnp.where(c < r, square, jnp.where(c == r, diagonal, zero))


def product(left, buf, tri, core, rows, reach, u, only):
    terms = [m for m in only if abs(u - m) <= 2]
    right = jnp.concatenate([block_of(buf, tri, m + 2 * SPAN + core, u - m + 2, rows) for m in terms], axis=0)
    low, high = terms[0] + reach, terms[-1] + reach
    return jnp.dot(left[:, low * rows : (high + 1) * rows], right, preferred_element_type=jnp.float32)


def gather_kernel(
    n, rows, adjacency, weight, t_low, partial, buf, adj, wgt, row, p_low, tri, via, p_early, t_early,
    send_sem, relay_sem, recv, pair_recv, via_recv, in_sem,
):
    me = lax.axis_index("blk")
    core = me % CORES
    place = (me // CORES) % PLANE
    group = me // (CORES * PLANE)
    groups = n // (CORES * PLANE)
    partner = me + 1 - 2 * core
    up = ((group + 1) % groups * PLANE + place) * CORES + core
    down = ((group + groups - 1) % groups * PLANE + place) * CORES + core
    x_mate = place + 1 - 2 * (place % 2)
    y_mate = (place + 2) % PLANE
    d_mate = SPAN - place
    inner = (place + 1) // 2 % 2

    def device(q):
        return (group * PLANE + q) * CORES + core

    def is_above(q, p):
        return (q - p + PLANE) // PLANE

    def cross(q, p):
        return q - p + PLANE - 2 * PLANE * is_above(q, p)

    def either(outer_one, inner_one):
        return outer_one + inner * (inner_one - outer_one)

    def slot(offset):
        return (offset + SPAN) * CORES + core

    total = buf.shape[1]
    bounds = [(s, e - s) for s, e in zip((0,) + CUTS, CUTS + (total,))]
    chunks = range(len(bounds))
    x_dev, y_dev = device(x_mate), device(y_mate)

    barrier = pltpu.get_barrier_semaphore()
    greeted = [partner, up, down, x_dev, y_dev]
    for other in greeted:
        pl.semaphore_signal(barrier, inc=1, device_id=(other,), device_id_type=MESH)

    step = rows // LOADS
    loads = []
    for i in range(LOADS):
        part = pl.ds(i * step, step)
        loads.append((
            pltpu.make_async_copy(adjacency.at[part], adj.at[part], in_sem.at[0, i]),
            pltpu.make_async_copy(weight.at[part], wgt.at[part], in_sem.at[1, i]),
        ))
    for pair_of in loads:
        for load in pair_of:
            load.start()

    center = slot(0)
    diagonal = jnp.zeros((1, rows), jnp.float32)
    for i, pair_of in enumerate(loads):
        for load in pair_of:
            load.wait()
        part = slice(i * step, (i + 1) * step)
        r = lax.broadcasted_iota(jnp.int32, (step, rows), 0) + i * step
        c = lax.broadcasted_iota(jnp.int32, (step, rows), 1)
        kept = []
        for k in range(5):
            cols = slice(k * rows, (k + 1) * rows)
            keep = adj[part, cols] == 1
            if k == 0:
                keep &= c >= r
            elif k == 2:
                keep |= c == r
            elif k == 4:
                keep &= c <= r
            kept.append(jnp.where(keep, wgt[part, cols].astype(jnp.float32), 0.0))
            row[part, cols] = kept[k].astype(row.dtype)
        packed = [jnp.where(c >= r, kept[0], kept[4])] + kept[1:4]
        for k in range(4):
            low = packed[k].astype(row.dtype)
            for h in range(2):
                start = (2 * k + h) * rows + i * step
                buf[center, start : start + step, :] = low[:, h * LANES : (h + 1) * LANES]
        diagonal += jnp.sum(jnp.where(c == r, kept[4], 0.0), axis=0, keepdims=True)
    tail = jnp.concatenate(
        [diagonal[:, :LANES], diagonal[:, LANES:], jnp.zeros((PAD - 2, LANES), jnp.float32)], axis=0
    )
    buf[center, 8 * rows :, :] = tail.astype(row.dtype)
    pl.semaphore_wait(barrier, len(greeted))

    def chunk(offset, j):
        return buf.at[slot(offset), pl.ds(bounds[j][0], bounds[j][1])]

    def arrival(offset, j):
        return recv.at[offset + SPAN - (offset + SPAN) // (SPAN + 1), j]

    def remote(source, target, sem, to):
        return pltpu.make_async_remote_copy(
            src_ref=source, dst_ref=target, send_sem=send_sem, recv_sem=sem, device_id=(to,), device_id_type=MESH
        )

    def send(offset, j, to, there):
        remote(chunk(offset, j), chunk(there, j), arrival(there, j), to).start()

    def pair(offset, j):
        remote(chunk(offset, j), chunk(offset, j), pair_recv.at[offset + SPAN], partner).start()

    def take(offset, j):
        pltpu.make_async_copy(chunk(0, j), chunk(offset, j), arrival(offset, j)).wait()

    def take_pair(offset, j):
        take(offset, j)
        pair(offset, j)

    def beyond(q):
        above = is_above(q, place)
        return above * up + (1 - above) * down

    def hop(q, j):
        send(q - place, j, beyond(q), cross(q, place))

    def other(offset):
        return slot(offset) + 1 - 2 * core

    def unpack(at):
        tri[at, 0], tri[at, 1] = ends_of(buf, at, rows)

    def unpack_own(offset):
        unpack(slot(offset))

    def unpack_other(offset):
        at = other(offset)
        pltpu.make_async_copy(buf.at[center], buf.at[at], pair_recv.at[offset + SPAN]).wait()
        unpack(at)

    x, y, d = (q - place for q in (x_mate, y_mate, d_mate))
    x_far, y_far, d_far = (cross(q, place) for q in (x_mate, y_mate, d_mate))
    near, far = either(d_far, d), either(d, d_far)

    remote(chunk(0, 0), via, via_recv, up + down - beyond(x_mate)).start()
    for j in chunks:
        send(0, j, y_dev, place - y_mate)
        send(0, j, x_dev, place - x_mate)
    for j in chunks:
        pair(0, j)
    unpack_own(0)
    def relay_far(j):
        take(y_far, j)
        send(y_far, j, x_dev, y_far + place - x_mate)
        pair(y_far, j)

    for j in chunks:
        take(y, j)
        hop(y_mate, j)
        pair(y, j)
        take(x, j)
        send(x, j, y_dev, x_mate - y_mate)
        pair(x, j)
        if j >= LAG:
            relay_far(j - LAG)
    for j in chunks[1:]:
        hop(x_mate, j)
    for j in chunks[-LAG:]:
        relay_far(j)
    pltpu.make_async_copy(chunk(0, 0), via, via_recv).wait()
    handed = cross(place, x_mate)
    relay = pltpu.make_async_remote_copy(
        src_ref=via, dst_ref=chunk(handed, 0), send_sem=relay_sem, recv_sem=arrival(handed, 0),
        device_id=(x_dev,), device_id_type=MESH,
    )
    relay.start()
    unpack_other(0)
    for offset in (x, y, y_far):
        unpack_own(offset)
        unpack_other(offset)
    sign = 1 - 2 * (place % 2)

    def width(i, reach):
        return pl.ds(pl.multiple_of((sign * i + reach) * rows, rows), rows)

    def toward(left, reach, u, terms):
        value = None
        for i in terms:
            at = sign * i + 2 * SPAN + core
            k = 2 + sign * (u - i)
            if abs(u - i) == 2:
                block = tri[at, k // 4]
            else:
                low = pl.multiple_of(2 * k * rows, rows)
                block = jnp.concatenate(
                    [buf[at, pl.ds(low, rows), :], buf[at, pl.ds(low + rows, rows), :]], axis=1
                )
            term = jnp.dot(left[:, width(i, reach)], block, preferred_element_type=jnp.float32)
            value = term if value is None else value + term
        return value

    p_scale = 1.0 / math.sqrt(B)
    t_scale = 1.0 / math.sqrt(B) / math.sqrt(2 * B)

    def near_to(u, least, most):
        return range(max(least, u - 2), min(most, u + 2) + 1)

    def put_p(u, value):
        p_low[:, width(u, 4)] = (value * p_scale).astype(p_low.dtype)

    def put_t(u, value):
        t_low[:, width(u, 6)] = (value * t_scale).astype(t_low.dtype)

    for u in range(2, 5):
        put_p(u, toward(row, 2, u, near_to(u, 0, 2)))
    for u in range(-2, 2):
        p_early[u + 2] = toward(row, 2, u, near_to(u, 0, 2))
    for u in range(4, 7):
        put_t(u, toward(p_low, 4, u, near_to(u, 2, 4)))
    for u in range(0, 4):
        t_early[u] = toward(p_low, 4, u, near_to(u, 2, 4))

    for j in chunks:
        take_pair(near, j)
    for offset, j in FORWARDS[0]:
        take_pair((far, x_far)[offset], j)
    unpack_own(near)
    unpack_other(near)

    for u in range(-4, 2):
        value = toward(row, 2, u, near_to(u, -2, -1))
        put_p(u, value + p_early[u + 2] if u >= -2 else value)
    for offset, j in FORWARDS[1]:
        take_pair((far, x_far)[offset], j)
    for u in range(-6, 4):
        value = toward(p_low, 4, u, near_to(u, -4, 1))
        put_t(u, value + t_early[u] if u >= 0 else value)
        for offset, j in FORWARDS_T.get(u, ()):
            take_pair((far, x_far)[offset], j)
    for u in range(-6, 7):
        partial[:, (u + 6) * rows : (u + 7) * rows] = product(t_low, buf, tri, core, rows, 6, u, range(-4, 5))
        for offset, j in FORWARDS_OUT.get(u, ()):
            take_pair((far, x_far)[offset], j)
    for offset in (far, x_far):
        pltpu.make_async_copy(buf.at[center], buf.at[other(offset)], pair_recv.at[offset + SPAN]).wait()
    blocks = buf.at[pl.ds(0, SENT_BLOCKS)]
    remote(blocks, blocks, pair_recv.at[0], partner).wait_send()
    relay.wait_send()


def last_kernel(rows, t_low, partial, buf, out, tri, stage, out_sem):
    core = lax.axis_index("blk") % CORES
    far = (-6, -5, 5, 6)
    middle = pl.ds(6 * rows, 5 * rows)
    writes = [pltpu.make_async_copy(partial.at[:, pl.ds(4 * rows, 5 * rows)], out.at[:, middle], out_sem.at[0])]
    writes[0].start()
    for i, m in enumerate(far):
        tri[i, 0], tri[i, 1] = ends_of(buf, m + 2 * SPAN + core, rows)
    for low, high in SPANS:
        for u in range(low, high):
            terms = [(i, m) for i, m in enumerate(far) if abs(u - m) <= 2]
            right = []
            for i, m in terms:
                k = u - m + 2
                at = m + 2 * SPAN + core
                right.append(tri[i, k // 4] if k in (0, 4) else block_of(buf, None, at, k, rows))
            first, last = terms[0][1] + 6, terms[-1][1] + 6
            value = jnp.dot(
                t_low[:, first * rows : (last + 1) * rows], jnp.concatenate(right, axis=0),
                preferred_element_type=jnp.float32,
            )
            if abs(u) <= 6:
                value += partial[:, (u + 6) * rows : (u + 7) * rows]
            stage[:, (u + 8) * rows : (u + 9) * rows] = value
        cols = pl.ds((low + 8) * rows, (high - low) * rows)
        write = pltpu.make_async_copy(stage.at[:, cols], out.at[:, cols], out_sem.at[len(writes)])
        write.start()
        writes.append(write)
    for write in writes:
        write.wait()


def local(n, adjacency, weight):
    rows = adjacency.shape[0]
    slots = (2 * SPAN + 1) * CORES
    low = weight.dtype
    chunks = len(CUTS) + 1
    vmem = pl.BlockSpec(memory_space=pltpu.VMEM)
    hbm = pl.BlockSpec(memory_space=pltpu.HBM)
    t_low, partial, buf = pl.pallas_call(
        functools.partial(gather_kernel, n, rows),
        out_shape=(
            jax.ShapeDtypeStruct((rows, 13 * rows), low),
            jax.ShapeDtypeStruct((rows, 13 * rows), jnp.float32),
            jax.ShapeDtypeStruct((slots, 8 * rows + PAD, LANES), low),
        ),
        in_specs=[hbm, hbm],
        out_specs=(vmem, vmem, vmem),
        scratch_shapes=[
            pltpu.VMEM(adjacency.shape, jnp.int32),
            pltpu.VMEM(weight.shape, low),
            pltpu.VMEM((rows, 5 * rows), low),
            pltpu.VMEM((rows, 9 * rows), low),
            pltpu.VMEM((slots, 2, rows, rows), low),
            pltpu.VMEM((CUTS[0], LANES), low),
            pltpu.VMEM((4, rows, rows), jnp.float32),
            pltpu.VMEM((4, rows, rows), jnp.float32),
            pltpu.SemaphoreType.DMA,
            pltpu.SemaphoreType.DMA,
            pltpu.SemaphoreType.DMA((2 * SPAN, chunks)),
            pltpu.SemaphoreType.DMA((2 * SPAN + 1,)),
            pltpu.SemaphoreType.DMA,
            pltpu.SemaphoreType.DMA((2, LOADS)),
        ],
        compiler_params=pltpu.CompilerParams(
            collective_id=0, has_side_effects=True, vmem_limit_bytes=24 * 1024 * 1024
        ),
        name="gather",
    )(*(pltpu.with_memory_space_constraint(x, pltpu.HBM) for x in (adjacency, weight)))
    return pl.pallas_call(
        functools.partial(last_kernel, rows),
        out_shape=jax.ShapeDtypeStruct((rows, 17 * rows), jnp.float32),
        in_specs=[vmem, vmem, vmem],
        out_specs=hbm,
        scratch_shapes=[
            pltpu.VMEM((4, 2, rows, rows), low),
            pltpu.VMEM((rows, 17 * rows), jnp.float32),
            pltpu.SemaphoreType.DMA((len(SPANS) + 1,)),
        ],
        compiler_params=pltpu.CompilerParams(vmem_limit_bytes=24 * 1024 * 1024),
        name="last",
    )(t_low, partial, buf)


def solution(mesh):
    in_specs = (P("blk", None), P("blk", None))
    out_specs = P("blk", None)
    n = mesh.shape["blk"]
    return jax.shard_map(
        functools.partial(local, n), mesh=mesh, in_specs=in_specs, out_specs=out_specs, check_vma=False
    )
```

```python
import functools
import math

import jax
import jax.numpy as jnp
from jax import lax
from jax.experimental import pallas as pl
from jax.experimental.pallas import tpu as pltpu
from jax.sharding import PartitionSpec as P

B = 512
MESH = pl.DeviceIdType.MESH
CORES = 2
PLANE = 4
SPAN = PLANE - 1
LANES = 128
PAD = 16
LOADS = 2
CUTS = (256, 640, 1024, 1408, 1792)
LAG = 2
SENT_BLOCKS = 2 + 2 + 2 + (2 * SPAN + 1)
FORWARDS = (
    ((0, 0), (0, 1), (0, 2), (1, 1), (1, 2)),
    ((0, 3), (0, 4), (0, 5), (1, 3)),
)
FORWARDS_T = {-1: ((1, 4),), 3: ((1, 0), (1, 5))}
FORWARDS_OUT = {}
SPANS = ((-8, -5), (-5, -2), (3, 6), (6, 9), (-2, 1), (1, 3))


def block_of(buf, tri, at, k, rows):
    if k in (0, 4):
        return tri[at, k // 4]
    low = 2 * k * rows
    return jnp.concatenate([buf[at, low : low + rows, :], buf[at, low + rows : low + 2 * rows, :]], axis=1)


def ends_of(buf, at, rows):
    r = lax.broadcasted_iota(jnp.int32, (rows, rows), 0)
    c = lax.broadcasted_iota(jnp.int32, (rows, rows), 1)
    square = jnp.concatenate([buf[at, :rows, :], buf[at, rows : 2 * rows, :]], axis=1)
    diagonal = jnp.concatenate(
        [buf[at, 8 * rows : 8 * rows + 1, :], buf[at, 8 * rows + 1 : 8 * rows + 2, :]], axis=1
    )
    zero = jnp.zeros_like(square)
    return jnp.where(c >= r, square, zero), jnp.where(c < r, square, jnp.where(c == r, diagonal, zero))


def product(left, buf, tri, core, rows, reach, u, only):
    terms = [m for m in only if abs(u - m) <= 2]
    right = jnp.concatenate([block_of(buf, tri, m + 2 * SPAN + core, u - m + 2, rows) for m in terms], axis=0)
    low, high = terms[0] + reach, terms[-1] + reach
    return jnp.dot(left[:, low * rows : (high + 1) * rows], right, preferred_element_type=jnp.float32)


def gather_kernel(
    n, rows, adjacency, weight, t_low, partial, buf, tri, adj, wgt, row, p_low, via, p_early, t_early,
    send_sem, relay_sem, recv, pair_recv, via_recv, in_sem,
):
    me = lax.axis_index("blk")
    core = me % CORES
    place = (me // CORES) % PLANE
    group = me // (CORES * PLANE)
    groups = n // (CORES * PLANE)
    partner = me + 1 - 2 * core
    up = ((group + 1) % groups * PLANE + place) * CORES + core
    down = ((group + groups - 1) % groups * PLANE + place) * CORES + core
    x_mate = place + 1 - 2 * (place % 2)
    y_mate = (place + 2) % PLANE
    d_mate = SPAN - place
    inner = (place + 1) // 2 % 2

    def device(q):
        return (group * PLANE + q) * CORES + core

    def is_above(q, p):
        return (q - p + PLANE) // PLANE

    def cross(q, p):
        return q - p + PLANE - 2 * PLANE * is_above(q, p)

    def either(outer_one, inner_one):
        return outer_one + inner * (inner_one - outer_one)

    def slot(offset):
        return (offset + SPAN) * CORES + core

    total = buf.shape[1]
    bounds = [(s, e - s) for s, e in zip((0,) + CUTS, CUTS + (total,))]
    chunks = range(len(bounds))
    x_dev, y_dev = device(x_mate), device(y_mate)

    barrier = pltpu.get_barrier_semaphore()
    greeted = [partner, up, down, x_dev, y_dev]
    for other in greeted:
        pl.semaphore_signal(barrier, inc=1, device_id=(other,), device_id_type=MESH)

    step = rows // LOADS
    loads = []
    for i in range(LOADS):
        part = pl.ds(i * step, step)
        loads.append((
            pltpu.make_async_copy(adjacency.at[part], adj.at[part], in_sem.at[0, i]),
            pltpu.make_async_copy(weight.at[part], wgt.at[part], in_sem.at[1, i]),
        ))
    for pair_of in loads:
        for load in pair_of:
            load.start()

    center = slot(0)
    diagonal = jnp.zeros((1, rows), jnp.float32)
    for i, pair_of in enumerate(loads):
        for load in pair_of:
            load.wait()
        part = slice(i * step, (i + 1) * step)
        r = lax.broadcasted_iota(jnp.int32, (step, rows), 0) + i * step
        c = lax.broadcasted_iota(jnp.int32, (step, rows), 1)
        kept = []
        for k in range(5):
            cols = slice(k * rows, (k + 1) * rows)
            keep = adj[part, cols] == 1
            if k == 0:
                keep &= c >= r
            elif k == 2:
                keep |= c == r
            elif k == 4:
                keep &= c <= r
            kept.append(jnp.where(keep, wgt[part, cols].astype(jnp.float32), 0.0))
            row[part, cols] = kept[k].astype(row.dtype)
        packed = [jnp.where(c >= r, kept[0], kept[4])] + kept[1:4]
        for k in range(4):
            low = packed[k].astype(row.dtype)
            for h in range(2):
                start = (2 * k + h) * rows + i * step
                buf[center, start : start + step, :] = low[:, h * LANES : (h + 1) * LANES]
        diagonal += jnp.sum(jnp.where(c == r, kept[4], 0.0), axis=0, keepdims=True)
    tail = jnp.concatenate(
        [diagonal[:, :LANES], diagonal[:, LANES:], jnp.zeros((PAD - 2, LANES), jnp.float32)], axis=0
    )
    buf[center, 8 * rows :, :] = tail.astype(row.dtype)
    pl.semaphore_wait(barrier, len(greeted))

    def chunk(offset, j):
        return buf.at[slot(offset), pl.ds(bounds[j][0], bounds[j][1])]

    def arrival(offset, j):
        return recv.at[offset + SPAN - (offset + SPAN) // (SPAN + 1), j]

    def remote(source, target, sem, to):
        return pltpu.make_async_remote_copy(
            src_ref=source, dst_ref=target, send_sem=send_sem, recv_sem=sem, device_id=(to,), device_id_type=MESH
        )

    def send(offset, j, to, there):
        remote(chunk(offset, j), chunk(there, j), arrival(there, j), to).start()

    def pair(offset, j):
        remote(chunk(offset, j), chunk(offset, j), pair_recv.at[offset + SPAN], partner).start()

    def take(offset, j):
        pltpu.make_async_copy(chunk(0, j), chunk(offset, j), arrival(offset, j)).wait()

    def take_pair(offset, j):
        take(offset, j)
        pair(offset, j)

    def beyond(q):
        above = is_above(q, place)
        return above * up + (1 - above) * down

    def hop(q, j):
        send(q - place, j, beyond(q), cross(q, place))

    def other(offset):
        return slot(offset) + 1 - 2 * core

    def unpack(at):
        tri[at, 0], tri[at, 1] = ends_of(buf, at, rows)

    def unpack_own(offset):
        unpack(slot(offset))

    def unpack_other(offset):
        at = other(offset)
        pltpu.make_async_copy(buf.at[center], buf.at[at], pair_recv.at[offset + SPAN]).wait()
        unpack(at)

    x, y, d = (q - place for q in (x_mate, y_mate, d_mate))
    x_far, y_far, d_far = (cross(q, place) for q in (x_mate, y_mate, d_mate))
    near, far = either(d_far, d), either(d, d_far)

    remote(chunk(0, 0), via, via_recv, up + down - beyond(x_mate)).start()
    for j in chunks:
        send(0, j, y_dev, place - y_mate)
        send(0, j, x_dev, place - x_mate)
    for j in chunks:
        pair(0, j)
    unpack_own(0)
    def relay_far(j):
        take(y_far, j)
        send(y_far, j, x_dev, y_far + place - x_mate)
        pair(y_far, j)

    for j in chunks:
        take(y, j)
        hop(y_mate, j)
        pair(y, j)
        take(x, j)
        send(x, j, y_dev, x_mate - y_mate)
        pair(x, j)
        if j >= LAG:
            relay_far(j - LAG)
    for j in chunks[1:]:
        hop(x_mate, j)
    for j in chunks[-LAG:]:
        relay_far(j)
    pltpu.make_async_copy(chunk(0, 0), via, via_recv).wait()
    handed = cross(place, x_mate)
    relay = pltpu.make_async_remote_copy(
        src_ref=via, dst_ref=chunk(handed, 0), send_sem=relay_sem, recv_sem=arrival(handed, 0),
        device_id=(x_dev,), device_id_type=MESH,
    )
    relay.start()
    unpack_other(0)
    for offset in (x, y, y_far):
        unpack_own(offset)
        unpack_other(offset)
    sign = 1 - 2 * (place % 2)

    def width(i, reach):
        return pl.ds(pl.multiple_of((sign * i + reach) * rows, rows), rows)

    def toward(left, reach, u, terms):
        value = None
        for i in terms:
            at = sign * i + 2 * SPAN + core
            k = 2 + sign * (u - i)
            if abs(u - i) == 2:
                block = tri[at, k // 4]
            else:
                low = pl.multiple_of(2 * k * rows, rows)
                block = jnp.concatenate(
                    [buf[at, pl.ds(low, rows), :], buf[at, pl.ds(low + rows, rows), :]], axis=1
                )
            term = jnp.dot(left[:, width(i, reach)], block, preferred_element_type=jnp.float32)
            value = term if value is None else value + term
        return value

    p_scale = 1.0 / math.sqrt(B)
    t_scale = 1.0 / math.sqrt(B) / math.sqrt(2 * B)

    def near_to(u, least, most):
        return range(max(least, u - 2), min(most, u + 2) + 1)

    def put_p(u, value):
        p_low[:, width(u, 4)] = (value * p_scale).astype(p_low.dtype)

    def put_t(u, value):
        t_low[:, width(u, 6)] = (value * t_scale).astype(t_low.dtype)

    for u in range(2, 5):
        put_p(u, toward(row, 2, u, near_to(u, 0, 2)))
    for u in range(-2, 2):
        p_early[u + 3] = toward(row, 2, u, near_to(u, 0, 2))
    for u in range(4, 7):
        put_t(u, toward(p_low, 4, u, near_to(u, 2, 4)))
    for u in range(0, 4):
        t_early[u] = toward(p_low, 4, u, near_to(u, 2, 4))

    for j in chunks:
        take_pair(near, j)
    for offset, j in FORWARDS[0]:
        take_pair((far, x_far)[offset], j)
    unpack_own(near)
    put_p(-4, toward(row, 2, -4, (-2,)))
    for u in range(-3, 1):
        value = toward(row, 2, u, (-2,))
        p_early[u + 3] = value + p_early[u + 3] if u > -3 else value
    put_t(-6, toward(p_low, 4, -6, (-4,)))
    for u in range(-5, -1):
        t_early[u + 9] = toward(p_low, 4, u, (-4,))
    unpack_other(near)

    for u in range(-3, 2):
        put_p(u, toward(row, 2, u, (-1,)) + p_early[u + 3])
    for offset, j in FORWARDS[1]:
        take_pair((far, x_far)[offset], j)
    for u in range(-5, 4):
        value = toward(p_low, 4, u, near_to(u, -3, 1))
        if u <= -2:
            value += t_early[u + 9]
        elif u >= 0:
            value += t_early[u]
        put_t(u, value)
        for offset, j in FORWARDS_T.get(u, ()):
            take_pair((far, x_far)[offset], j)
    for u in (*range(-6, -2), *range(3, 7)):
        partial[:, (u + 6) * rows : (u + 7) * rows] = product(t_low, buf, tri, core, rows, 6, u, range(-4, 5))
        for offset, j in FORWARDS_OUT.get(u, ()):
            take_pair((far, x_far)[offset], j)
    for offset in (far, x_far):
        pltpu.make_async_copy(buf.at[center], buf.at[other(offset)], pair_recv.at[offset + SPAN]).wait()
    blocks = buf.at[pl.ds(0, SENT_BLOCKS)]
    remote(blocks, blocks, pair_recv.at[0], partner).wait_send()
    relay.wait_send()


def last_kernel(rows, t_low, partial, buf, tri, out, far_tri, stage, out_sem):
    core = lax.axis_index("blk") % CORES
    far = (-6, -5, 5, 6)
    writes = []
    for i, m in enumerate(far):
        far_tri[i, 0], far_tri[i, 1] = ends_of(buf, m + 2 * SPAN + core, rows)
    for low, high in SPANS:
        for u in range(low, high):
            if abs(u) <= 2:
                stage[:, (u + 8) * rows : (u + 9) * rows] = product(
                    t_low, buf, tri, core, rows, 6, u, range(-4, 5)
                )
                continue
            terms = [(i, m) for i, m in enumerate(far) if abs(u - m) <= 2]
            right = []
            for i, m in terms:
                k = u - m + 2
                at = m + 2 * SPAN + core
                right.append(far_tri[i, k // 4] if k in (0, 4) else block_of(buf, None, at, k, rows))
            first, last = terms[0][1] + 6, terms[-1][1] + 6
            value = jnp.dot(
                t_low[:, first * rows : (last + 1) * rows], jnp.concatenate(right, axis=0),
                preferred_element_type=jnp.float32,
            )
            if abs(u) <= 6:
                value += partial[:, (u + 6) * rows : (u + 7) * rows]
            stage[:, (u + 8) * rows : (u + 9) * rows] = value
        cols = pl.ds((low + 8) * rows, (high - low) * rows)
        write = pltpu.make_async_copy(stage.at[:, cols], out.at[:, cols], out_sem.at[len(writes)])
        write.start()
        writes.append(write)
    for write in writes:
        write.wait()


def local(n, adjacency, weight):
    rows = adjacency.shape[0]
    slots = (2 * SPAN + 1) * CORES
    low = weight.dtype
    chunks = len(CUTS) + 1
    vmem = pl.BlockSpec(memory_space=pltpu.VMEM)
    hbm = pl.BlockSpec(memory_space=pltpu.HBM)
    t_low, partial, buf, tri = pl.pallas_call(
        functools.partial(gather_kernel, n, rows),
        out_shape=(
            jax.ShapeDtypeStruct((rows, 13 * rows), low),
            jax.ShapeDtypeStruct((rows, 13 * rows), jnp.float32),
            jax.ShapeDtypeStruct((slots, 8 * rows + PAD, LANES), low),
            jax.ShapeDtypeStruct((slots, 2, rows, rows), low),
        ),
        in_specs=[hbm, hbm],
        out_specs=(vmem, vmem, vmem, vmem),
        scratch_shapes=[
            pltpu.VMEM(adjacency.shape, jnp.int32),
            pltpu.VMEM(weight.shape, low),
            pltpu.VMEM((rows, 5 * rows), low),
            pltpu.VMEM((rows, 9 * rows), low),
            pltpu.VMEM((CUTS[0], LANES), low),
            pltpu.VMEM((5, rows, rows), jnp.float32),
            pltpu.VMEM((8, rows, rows), jnp.float32),
            pltpu.SemaphoreType.DMA,
            pltpu.SemaphoreType.DMA,
            pltpu.SemaphoreType.DMA((2 * SPAN, chunks)),
            pltpu.SemaphoreType.DMA((2 * SPAN + 1,)),
            pltpu.SemaphoreType.DMA,
            pltpu.SemaphoreType.DMA((2, LOADS)),
        ],
        compiler_params=pltpu.CompilerParams(
            collective_id=0, has_side_effects=True, vmem_limit_bytes=24 * 1024 * 1024
        ),
        name="gather",
    )(*(pltpu.with_memory_space_constraint(x, pltpu.HBM) for x in (adjacency, weight)))
    return pl.pallas_call(
        functools.partial(last_kernel, rows),
        out_shape=jax.ShapeDtypeStruct((rows, 17 * rows), jnp.float32),
        in_specs=[vmem, vmem, vmem, vmem],
        out_specs=hbm,
        scratch_shapes=[
            pltpu.VMEM((4, 2, rows, rows), low),
            pltpu.VMEM((rows, 17 * rows), jnp.float32),
            pltpu.SemaphoreType.DMA((len(SPANS),)),
        ],
        compiler_params=pltpu.CompilerParams(vmem_limit_bytes=24 * 1024 * 1024),
        name="last",
    )(t_low, partial, buf, tri)


def solution(mesh):
    in_specs = (P("blk", None), P("blk", None))
    out_specs = P("blk", None)
    n = mesh.shape["blk"]
    return jax.shard_map(
        functools.partial(local, n), mesh=mesh, in_specs=in_specs, out_specs=out_specs, check_vma=False
    )
```

```python
import functools
import math

import jax
import jax.numpy as jnp
from jax import lax
from jax.experimental import pallas as pl
from jax.experimental.pallas import tpu as pltpu
from jax.sharding import PartitionSpec as P

B = 512
MESH = pl.DeviceIdType.MESH
CORES = 2
PLANE = 4
SPAN = PLANE - 1
LANES = 128
PAD = 16
LOADS = 2
CUTS = (256, 640, 1024, 1408, 1792)
LAG = 3
SENT_BLOCKS = 2 + 2 + 2 + (2 * SPAN + 1)
FORWARDS = (
    ((0, 0), (0, 1), (0, 2), (1, 1), (1, 2)),
    ((0, 3), (0, 4), (0, 5), (1, 3)),
)
FORWARDS_T = {-1: ((1, 4),), 3: ((1, 0), (1, 5))}
FORWARDS_OUT = {}
SPANS = ((-8, -5), (-5, -2), (3, 6), (6, 9), (-2, 1), (1, 3))


def block_of(buf, tri, at, k, rows):
    if k in (0, 4):
        return tri[at, k // 4]
    low = 2 * k * rows
    return jnp.concatenate([buf[at, low : low + rows, :], buf[at, low + rows : low + 2 * rows, :]], axis=1)


def ends_of(buf, at, rows):
    r = lax.broadcasted_iota(jnp.int32, (rows, rows), 0)
    c = lax.broadcasted_iota(jnp.int32, (rows, rows), 1)
    square = jnp.concatenate([buf[at, :rows, :], buf[at, rows : 2 * rows, :]], axis=1)
    diagonal = jnp.concatenate(
        [buf[at, 8 * rows : 8 * rows + 1, :], buf[at, 8 * rows + 1 : 8 * rows + 2, :]], axis=1
    )
    zero = jnp.zeros_like(square)
    return jnp.where(c >= r, square, zero), jnp.where(c < r, square, jnp.where(c == r, diagonal, zero))


def product(left, buf, tri, core, rows, reach, u, only):
    terms = [m for m in only if abs(u - m) <= 2]
    right = jnp.concatenate([block_of(buf, tri, m + 2 * SPAN + core, u - m + 2, rows) for m in terms], axis=0)
    low, high = terms[0] + reach, terms[-1] + reach
    return jnp.dot(left[:, low * rows : (high + 1) * rows], right, preferred_element_type=jnp.float32)


def gather_kernel(
    n, rows, adjacency, weight, t_low, partial, buf, tri, adj, wgt, row, p_low, via, p_early, t_early,
    send_sem, relay_sem, recv, pair_recv, via_recv, in_sem,
):
    me = lax.axis_index("blk")
    core = me % CORES
    place = (me // CORES) % PLANE
    group = me // (CORES * PLANE)
    groups = n // (CORES * PLANE)
    partner = me + 1 - 2 * core
    up = ((group + 1) % groups * PLANE + place) * CORES + core
    down = ((group + groups - 1) % groups * PLANE + place) * CORES + core
    x_mate = place + 1 - 2 * (place % 2)
    y_mate = (place + 2) % PLANE
    d_mate = SPAN - place
    inner = (place + 1) // 2 % 2

    def device(q):
        return (group * PLANE + q) * CORES + core

    def is_above(q, p):
        return (q - p + PLANE) // PLANE

    def cross(q, p):
        return q - p + PLANE - 2 * PLANE * is_above(q, p)

    def either(outer_one, inner_one):
        return outer_one + inner * (inner_one - outer_one)

    def slot(offset):
        return (offset + SPAN) * CORES + core

    total = buf.shape[1]
    bounds = [(s, e - s) for s, e in zip((0,) + CUTS, CUTS + (total,))]
    chunks = range(len(bounds))
    x_dev, y_dev = device(x_mate), device(y_mate)

    barrier = pltpu.get_barrier_semaphore()
    greeted = [partner, up, down, x_dev, y_dev]
    for other in greeted:
        pl.semaphore_signal(barrier, inc=1, device_id=(other,), device_id_type=MESH)

    step = rows // LOADS
    loads = []
    for i in range(LOADS):
        part = pl.ds(i * step, step)
        loads.append((
            pltpu.make_async_copy(adjacency.at[part], adj.at[part], in_sem.at[0, i]),
            pltpu.make_async_copy(weight.at[part], wgt.at[part], in_sem.at[1, i]),
        ))
    for pair_of in loads:
        for load in pair_of:
            load.start()

    center = slot(0)
    diagonal = jnp.zeros((1, rows), jnp.float32)
    for i, pair_of in enumerate(loads):
        for load in pair_of:
            load.wait()
        part = slice(i * step, (i + 1) * step)
        r = lax.broadcasted_iota(jnp.int32, (step, rows), 0) + i * step
        c = lax.broadcasted_iota(jnp.int32, (step, rows), 1)
        kept = []
        for k in range(5):
            cols = slice(k * rows, (k + 1) * rows)
            keep = adj[part, cols] == 1
            if k == 0:
                keep &= c >= r
            elif k == 2:
                keep |= c == r
            elif k == 4:
                keep &= c <= r
            kept.append(jnp.where(keep, wgt[part, cols].astype(jnp.float32), 0.0))
            row[part, cols] = kept[k].astype(row.dtype)
        packed = [jnp.where(c >= r, kept[0], kept[4])] + kept[1:4]
        for k in range(4):
            low = packed[k].astype(row.dtype)
            for h in range(2):
                start = (2 * k + h) * rows + i * step
                buf[center, start : start + step, :] = low[:, h * LANES : (h + 1) * LANES]
        diagonal += jnp.sum(jnp.where(c == r, kept[4], 0.0), axis=0, keepdims=True)
    tail = jnp.concatenate(
        [diagonal[:, :LANES], diagonal[:, LANES:], jnp.zeros((PAD - 2, LANES), jnp.float32)], axis=0
    )
    buf[center, 8 * rows :, :] = tail.astype(row.dtype)
    pl.semaphore_wait(barrier, len(greeted))

    def chunk(offset, j):
        return buf.at[slot(offset), pl.ds(bounds[j][0], bounds[j][1])]

    def arrival(offset, j):
        return recv.at[offset + SPAN - (offset + SPAN) // (SPAN + 1), j]

    def remote(source, target, sem, to):
        return pltpu.make_async_remote_copy(
            src_ref=source, dst_ref=target, send_sem=send_sem, recv_sem=sem, device_id=(to,), device_id_type=MESH
        )

    def send(offset, j, to, there):
        remote(chunk(offset, j), chunk(there, j), arrival(there, j), to).start()

    def pair(offset, j):
        remote(chunk(offset, j), chunk(offset, j), pair_recv.at[offset + SPAN], partner).start()

    def take(offset, j):
        pltpu.make_async_copy(chunk(0, j), chunk(offset, j), arrival(offset, j)).wait()

    def take_pair(offset, j):
        take(offset, j)
        pair(offset, j)

    def beyond(q):
        above = is_above(q, place)
        return above * up + (1 - above) * down

    def hop(q, j):
        send(q - place, j, beyond(q), cross(q, place))

    def other(offset):
        return slot(offset) + 1 - 2 * core

    def unpack(at):
        tri[at, 0], tri[at, 1] = ends_of(buf, at, rows)

    def unpack_own(offset):
        unpack(slot(offset))

    def unpack_other(offset):
        at = other(offset)
        pltpu.make_async_copy(buf.at[center], buf.at[at], pair_recv.at[offset + SPAN]).wait()
        unpack(at)

    x, y, d = (q - place for q in (x_mate, y_mate, d_mate))
    x_far, y_far, d_far = (cross(q, place) for q in (x_mate, y_mate, d_mate))
    near, far = either(d_far, d), either(d, d_far)

    remote(chunk(0, 0), via, via_recv, up + down - beyond(x_mate)).start()
    for j in chunks:
        send(0, j, y_dev, place - y_mate)
        send(0, j, x_dev, place - x_mate)
    for j in chunks:
        pair(0, j)
    unpack_own(0)
    def relay_far(j):
        take(y_far, j)
        send(y_far, j, x_dev, y_far + place - x_mate)
        pair(y_far, j)

    for j in chunks:
        take(y, j)
        hop(y_mate, j)
        pair(y, j)
        take(x, j)
        send(x, j, y_dev, x_mate - y_mate)
        pair(x, j)
        if j >= LAG:
            relay_far(j - LAG)
    for j in chunks[1:]:
        hop(x_mate, j)
    for j in chunks[-LAG:]:
        relay_far(j)
    pltpu.make_async_copy(chunk(0, 0), via, via_recv).wait()
    handed = cross(place, x_mate)
    relay = pltpu.make_async_remote_copy(
        src_ref=via, dst_ref=chunk(handed, 0), send_sem=relay_sem, recv_sem=arrival(handed, 0),
        device_id=(x_dev,), device_id_type=MESH,
    )
    relay.start()
    unpack_other(0)
    for offset in (x, y, y_far):
        unpack_own(offset)
        unpack_other(offset)
    sign = 1 - 2 * (place % 2)

    def width(i, reach):
        return pl.ds(pl.multiple_of((sign * i + reach) * rows, rows), rows)

    def toward(left, reach, u, terms):
        value = None
        for i in terms:
            at = sign * i + 2 * SPAN + core
            k = 2 + sign * (u - i)
            if abs(u - i) == 2:
                block = tri[at, k // 4]
            else:
                low = pl.multiple_of(2 * k * rows, rows)
                block = jnp.concatenate(
                    [buf[at, pl.ds(low, rows), :], buf[at, pl.ds(low + rows, rows), :]], axis=1
                )
            term = jnp.dot(left[:, width(i, reach)], block, preferred_element_type=jnp.float32)
            value = term if value is None else value + term
        return value

    p_scale = 1.0 / math.sqrt(B)
    t_scale = 1.0 / math.sqrt(B) / math.sqrt(2 * B)

    def near_to(u, least, most):
        return range(max(least, u - 2), min(most, u + 2) + 1)

    def put_p(u, value):
        p_low[:, width(u, 4)] = (value * p_scale).astype(p_low.dtype)

    def put_t(u, value):
        t_low[:, width(u, 6)] = (value * t_scale).astype(t_low.dtype)

    for u in range(2, 5):
        put_p(u, toward(row, 2, u, near_to(u, 0, 2)))
    for u in range(-2, 2):
        p_early[u + 3] = toward(row, 2, u, near_to(u, 0, 2))
    for u in range(4, 7):
        put_t(u, toward(p_low, 4, u, near_to(u, 2, 4)))
    for u in range(0, 4):
        t_early[u] = toward(p_low, 4, u, near_to(u, 2, 4))

    for j in chunks:
        take_pair(near, j)
    for offset, j in FORWARDS[0]:
        take_pair((far, x_far)[offset], j)
    unpack_own(near)
    put_p(-4, toward(row, 2, -4, (-2,)))
    for u in range(-3, 1):
        value = toward(row, 2, u, (-2,))
        p_early[u + 3] = value + p_early[u + 3] if u > -3 else value
    put_t(-6, toward(p_low, 4, -6, (-4,)))
    for u in range(-5, -1):
        t_early[u + 9] = toward(p_low, 4, u, (-4,))
    unpack_other(near)

    for u in range(-3, 2):
        put_p(u, toward(row, 2, u, (-1,)) + p_early[u + 3])
    for offset, j in FORWARDS[1]:
        take_pair((far, x_far)[offset], j)
    for u in range(-5, 4):
        value = toward(p_low, 4, u, near_to(u, -3, 1))
        if u <= -2:
            value += t_early[u + 9]
        elif u >= 0:
            value += t_early[u]
        put_t(u, value)
        for offset, j in FORWARDS_T.get(u, ()):
            take_pair((far, x_far)[offset], j)
    for u in (*range(-6, -2), *range(3, 7)):
        partial[:, (u + 6) * rows : (u + 7) * rows] = product(t_low, buf, tri, core, rows, 6, u, range(-4, 5))
        for offset, j in FORWARDS_OUT.get(u, ()):
            take_pair((far, x_far)[offset], j)
    for offset in (far, x_far):
        pltpu.make_async_copy(buf.at[center], buf.at[other(offset)], pair_recv.at[offset + SPAN]).wait()
    blocks = buf.at[pl.ds(0, SENT_BLOCKS)]
    remote(blocks, blocks, pair_recv.at[0], partner).wait_send()
    relay.wait_send()


def last_kernel(rows, t_low, partial, buf, tri, out, far_tri, stage, out_sem):
    core = lax.axis_index("blk") % CORES
    far = (-6, -5, 5, 6)
    writes = []
    for i, m in enumerate(far):
        far_tri[i, 0], far_tri[i, 1] = ends_of(buf, m + 2 * SPAN + core, rows)
    for low, high in SPANS:
        for u in range(low, high):
            if abs(u) <= 2:
                stage[:, (u + 8) * rows : (u + 9) * rows] = product(
                    t_low, buf, tri, core, rows, 6, u, range(-4, 5)
                )
                continue
            terms = [(i, m) for i, m in enumerate(far) if abs(u - m) <= 2]
            right = []
            for i, m in terms:
                k = u - m + 2
                at = m + 2 * SPAN + core
                right.append(far_tri[i, k // 4] if k in (0, 4) else block_of(buf, None, at, k, rows))
            first, last = terms[0][1] + 6, terms[-1][1] + 6
            value = jnp.dot(
                t_low[:, first * rows : (last + 1) * rows], jnp.concatenate(right, axis=0),
                preferred_element_type=jnp.float32,
            )
            if abs(u) <= 6:
                value += partial[:, (u + 6) * rows : (u + 7) * rows]
            stage[:, (u + 8) * rows : (u + 9) * rows] = value
        cols = pl.ds((low + 8) * rows, (high - low) * rows)
        write = pltpu.make_async_copy(stage.at[:, cols], out.at[:, cols], out_sem.at[len(writes)])
        write.start()
        writes.append(write)
    for write in writes:
        write.wait()


def local(n, adjacency, weight):
    rows = adjacency.shape[0]
    slots = (2 * SPAN + 1) * CORES
    low = weight.dtype
    chunks = len(CUTS) + 1
    vmem = pl.BlockSpec(memory_space=pltpu.VMEM)
    hbm = pl.BlockSpec(memory_space=pltpu.HBM)
    t_low, partial, buf, tri = pl.pallas_call(
        functools.partial(gather_kernel, n, rows),
        out_shape=(
            jax.ShapeDtypeStruct((rows, 13 * rows), low),
            jax.ShapeDtypeStruct((rows, 13 * rows), jnp.float32),
            jax.ShapeDtypeStruct((slots, 8 * rows + PAD, LANES), low),
            jax.ShapeDtypeStruct((slots, 2, rows, rows), low),
        ),
        in_specs=[hbm, hbm],
        out_specs=(vmem, vmem, vmem, vmem),
        scratch_shapes=[
            pltpu.VMEM(adjacency.shape, jnp.int32),
            pltpu.VMEM(weight.shape, low),
            pltpu.VMEM((rows, 5 * rows), low),
            pltpu.VMEM((rows, 9 * rows), low),
            pltpu.VMEM((CUTS[0], LANES), low),
            pltpu.VMEM((5, rows, rows), jnp.float32),
            pltpu.VMEM((8, rows, rows), jnp.float32),
            pltpu.SemaphoreType.DMA,
            pltpu.SemaphoreType.DMA,
            pltpu.SemaphoreType.DMA((2 * SPAN, chunks)),
            pltpu.SemaphoreType.DMA((2 * SPAN + 1,)),
            pltpu.SemaphoreType.DMA,
            pltpu.SemaphoreType.DMA((2, LOADS)),
        ],
        compiler_params=pltpu.CompilerParams(
            collective_id=0, has_side_effects=True, vmem_limit_bytes=24 * 1024 * 1024
        ),
        name="gather",
    )(*(pltpu.with_memory_space_constraint(x, pltpu.HBM) for x in (adjacency, weight)))
    return pl.pallas_call(
        functools.partial(last_kernel, rows),
        out_shape=jax.ShapeDtypeStruct((rows, 17 * rows), jnp.float32),
        in_specs=[vmem, vmem, vmem, vmem],
        out_specs=hbm,
        scratch_shapes=[
            pltpu.VMEM((4, 2, rows, rows), low),
            pltpu.VMEM((rows, 17 * rows), jnp.float32),
            pltpu.SemaphoreType.DMA((len(SPANS),)),
        ],
        compiler_params=pltpu.CompilerParams(vmem_limit_bytes=24 * 1024 * 1024),
        name="last",
    )(t_low, partial, buf, tri)


def solution(mesh):
    in_specs = (P("blk", None), P("blk", None))
    out_specs = P("blk", None)
    n = mesh.shape["blk"]
    return jax.shard_map(
        functools.partial(local, n), mesh=mesh, in_specs=in_specs, out_specs=out_specs, check_vma=False
    )
```
